32 devices in a mesh: groups: 2 (over y), gx: 4 (over z), gy: 2 (over x), gz: 2 (over core).
Axes of the slice: x: 2, y: 2, z: 4, core: 2. Of those that a mesh axis runs over, the one named last changes fastest.
Arguments:
- pair: float32 [256, 48, 48], P(('groups', 'gz'), 'gx', 'gy'), parts along dimension 0, may hold values from -6 to 6
- residue_mask: int32 [96], P('groups'), parts along dimension 0, may hold values 0 or 1
- norm_in_gain: float32 [2, 128], P(None, 'gz'), may hold values from 0.25 to 1.75
- proj_weight: bfloat16 [2, 4, 128, 128], P(None, None, None, 'gz'), may hold values from -0.5 to 0.5
- gate_weight: bfloat16 [2, 128, 128], P(None, None, 'gz'), may hold values from -0.5 to 0.5
- norm_out_gain: float32 [2, 128], P(None, 'gz'), may hold values from 0.25 to 1.75
- out_weight: bfloat16 [2, 128, 128], P(None, None, 'gz'), may hold values from -0.5 to 0.5
Outputs:
- pair_out: float32 [256, 48, 48], P(('groups', 'gz'), 'gx', 'gy'), parts along dimension 0
The draws below stay inside these ranges and needn't reach their ends.
There are 2 independent parts, one for each index of `groups`. The reference program is written for one: setup_inputs(seed, part) draws one part's arguments, and reference() takes and returns one part's arrays. A program takes and returns all parts, laid end to end along the dimension named above; an argument that names none is the same for every part. Nothing has to cross between parts.
All inputs are finite; a program needn't handle non-finite values.
Results may differ from the reference program's by a relative error of at most 0.006.
Values may be sent and summed in bfloat16 or wider, within the bound.
A program may use at most 64 MiB of HBM per device.

```python
import jax
import jax.numpy as jnp
from jax import lax

CHANNELS = 128
HIDDEN_SIZE = 128
RES = 48


def with_ends(entries, stream_key, smallest, top_value):
    extent = entries.shape
    index_at = [jax.random.randint(jax.random.fold_in(stream_key, axis), (), 0, extent[axis]) for axis in range(len(extent))]
    entries = entries.at[tuple(index_at)].set(smallest)
    longest = extent.index(max(extent))
    index_at[longest] = (index_at[longest] + 1) % extent[longest]
    return entries.at[tuple(index_at)].set(top_value)


def block_levels(rng, dims, split, least, largest):
    loudness = 1.0
    for dim, shards_of in split:
        heights = jax.random.uniform(jax.random.fold_in(jax.random.fold_in(rng, 6), dim), (shards_of,), jnp.float32, least / len(split), largest / len(split))
        loudness = loudness * jnp.repeat(jnp.exp(heights), dims[dim] // shards_of).reshape((-1,) + (1,) * (len(dims) - 1 - dim))
    return loudness


def gaussian(stream_key, shape, deviation, bound, cuts=(), dtype=jnp.bfloat16):
    result = jax.random.normal(stream_key, shape, jnp.float32) * deviation
    if len(cuts) > 0:
        result = block_levels(stream_key, shape, cuts, -0.22, 0.18) * result
    return jnp.clip(result, min=-bound, max=bound).astype(dtype)


def setup_inputs(seed: int = 0, part: int = 0) -> dict:
    key_of = jax.random.split(jax.random.key(seed), 8)
    own_keys = jax.random.split(jax.random.fold_in(key_of[7], part), 8)
    return {
        "pair": gaussian(own_keys[0], (CHANNELS, RES, RES), 1.0, 6.0, ((0, 2), (1, 4), (2, 2)), jnp.float32),
        "residue_mask": with_ends((jax.random.randint(own_keys[1], (RES,), 0, 4) < 3).astype(jnp.int32), jax.random.fold_in(own_keys[1], 1), 0, 1),
        "norm_in_gain": jnp.clip(1.0 + 0.15 * jax.random.normal(key_of[2], (2, CHANNELS), jnp.float32), 0.25, 1.75),
        "proj_weight": gaussian(key_of[3], (2, 4, CHANNELS, HIDDEN_SIZE), CHANNELS ** -0.5, 0.5, ((3, 2),)),
        "gate_weight": gaussian(key_of[4], (2, CHANNELS, CHANNELS), CHANNELS ** -0.5, 0.5, ((2, 2),)),
        "norm_out_gain": jnp.clip(1.0 + 0.15 * jax.random.normal(key_of[5], (2, HIDDEN_SIZE), jnp.float32), 0.25, 1.75),
        "out_weight": gaussian(key_of[6], (2, HIDDEN_SIZE, CHANNELS), HIDDEN_SIZE ** -0.5, 0.5, ((2, 2),)),
    }


EPSILON = 1e-05

def layer_norm(values, gain_row):
    mean_val = lax.optimization_barrier(jnp.mean(values, axis=0))
    centred = values - mean_val
    spread = lax.optimization_barrier(jnp.mean(centred * centred, axis=0))
    normed = (centred * lax.rsqrt(spread + EPSILON) * gain_row[:, None, None]).astype(jnp.bfloat16)
    return lax.optimization_barrier(normed).astype(jnp.float32)

def reference(pair, residue_mask, norm_in_gain, proj_weight, gate_weight, norm_out_gain, out_weight):
    residue_flags = residue_mask.astype(jnp.float32)
    pair_mask = residue_flags[:, None] * residue_flags[None, :]
    current = pair
    for update in range(2):
        normed = layer_norm(current, norm_in_gain[update])

        def project(which_one):
            return jnp.einsum('cij,ch->hij', normed, proj_weight[update, which_one].astype(jnp.float32))
        left = (jax.nn.sigmoid(project(0)) * project(1) * pair_mask).astype(jnp.bfloat16)
        left = lax.optimization_barrier(left).astype(jnp.float32)
        right = (jax.nn.sigmoid(project(2)) * project(3) * pair_mask).astype(jnp.bfloat16)
        right = lax.optimization_barrier(right).astype(jnp.float32)
        gate_values = jax.nn.sigmoid(jnp.einsum('cij,cd->dij', normed, gate_weight[update].astype(jnp.float32)))
        if update == 0:
            triangle = jnp.einsum('hik,hjk->hij', left, right)
        else:
            triangle = jnp.einsum('hki,hkj->hij', left, right)
        tri_normed = layer_norm(triangle, norm_out_gain[update])
        current = current + gate_values * jnp.einsum('hij,hd->dij', tri_normed, out_weight[update].astype(jnp.float32))
    return current
```

```python
import functools

import jax
import jax.numpy as jnp
from jax import lax
from jax.experimental import pallas as pl
from jax.experimental.pallas import tpu as pltpu
from jax.sharding import PartitionSpec as P

EPSILON = 1e-05


def layer_norm_gathered(values, gain_part):
    full_values, full_gain = (
        lax.all_gather(values, "gz", axis=0, tiled=True),
        lax.all_gather(gain_part, "gz", axis=0, tiled=True),
    )
    mean_val = jnp.mean(full_values, axis=0)
    centred = full_values - mean_val
    spread = jnp.mean(centred * centred, axis=0)
    result = (centred * lax.rsqrt(spread + EPSILON) * full_gain[:, None, None]).astype(jnp.bfloat16)
    return result


def transpose_tile(pair_tile):
    depth_dim, tile_rows, tile_cols = pair_tile.shape
    across = lax.axis_size("gy")
    down_size = lax.axis_size("gx")
    quarter = tile_rows // across
    spread_rows = lax.all_to_all(pair_tile, "gy", split_axis=1, concat_axis=2, tiled=True)
    blocks = spread_rows.reshape(depth_dim, quarter, down_size, tile_rows)
    blocks = jnp.transpose(blocks, (0, 3, 2, 1))[:, :, :, None, :]
    moved_back = lax.all_to_all(
        lax.all_to_all(blocks, "gx", split_axis=2, concat_axis=2, tiled=True),
        "gy",
        split_axis=2,
        concat_axis=3,
        tiled=True,
    )
    return moved_back.reshape(depth_dim, tile_rows, tile_cols)


def fold_panels(left_tile, right_tile):
    left_panel = lax.all_gather(left_tile, "gy", axis=2, tiled=True)
    return jnp.einsum(
        "hik,hkj->hij",
        left_panel,
        lax.all_gather(right_tile, "gx", axis=1, tiled=True),
        preferred_element_type=jnp.float32,
    )


def per_device(
    pair, residue_mask, norm_in_gain, proj_weight, gate_weight, norm_out_gain, out_weight
):
    tile_rows = pair.shape[1]
    tile_cols = pair.shape[2]
    row_start = lax.axis_index("gx") * tile_rows
    col_start = lax.axis_index("gy") * tile_cols
    row_flags = lax.dynamic_slice_in_dim(residue_mask, row_start, tile_rows).astype(jnp.float32)
    col_flags = lax.dynamic_slice_in_dim(residue_mask, col_start, tile_cols).astype(jnp.float32)
    pair_mask = row_flags[:, None] * col_flags[None, :]
    current = pair
    for update in range(2):
        normed = layer_norm_gathered(current, norm_in_gain[update])
        projected = jnp.einsum(
            "cij,pch->phij", normed, proj_weight[update], preferred_element_type=jnp.float32
        )
        left_tile = (jax.nn.sigmoid(projected[0]) * projected[1] * pair_mask).astype(jnp.bfloat16)
        right_tile = (jax.nn.sigmoid(projected[2]) * projected[3] * pair_mask).astype(jnp.bfloat16)
        gate_values = jax.nn.sigmoid(
            jnp.einsum(
                "cij,cd->dij", normed, gate_weight[update], preferred_element_type=jnp.float32
            )
        )
        if update == 0:
            triangle = fold_panels(left_tile, transpose_tile(right_tile))
        else:
            triangle = fold_panels(transpose_tile(left_tile), right_tile)
        tri_normed = layer_norm_gathered(triangle, norm_out_gain[update])
        current = current + gate_values * jnp.einsum(
            "hij,hd->dij", tri_normed, out_weight[update], preferred_element_type=jnp.float32
        )
    return current


MESH_ID = pl.DeviceIdType.MESH


def channel_norm(values, gain_row):
    mean_val = jnp.mean(values, axis=1, keepdims=True)
    centred = values - mean_val
    spread = jnp.mean(centred * centred, axis=1, keepdims=True)
    return (centred * lax.rsqrt(spread + EPSILON) * gain_row).astype(jnp.bfloat16)


def rows_dot(rows, weight_t):
    return lax.dot_general(
        rows, weight_t, (((1,), (1,)), ((), ())), preferred_element_type=jnp.float32
    )


def fused_kernel(
    sizes, x_ref, w_ref, g_ref, m_ref, o_ref,
    x_all, w_all, g_in, l_send, r_send, l_got, r_got, l_wide, r_wide, turn_a, turn_b, z_t,
    s_sem, x_sem, ls_sem, rs_sem, lr_sem, rr_sem, copy_sem,
):
    n_gx, n_gy, n_gz, side = sizes
    n_q = n_gy * n_gz
    row_id, gy_id, gz_id = lax.axis_index("gx"), lax.axis_index("gy"), lax.axis_index("gz")
    col_id = gy_id * n_gz + gz_id
    other = 1 - gz_id
    half = w_ref.shape[2]
    on_diag = row_id == col_id

    def device(at_row, at_col):
        return {"gx": at_row, "gy": at_col // n_gz, "gz": lax.rem(at_col, n_gz)}

    barrier = pltpu.get_barrier_semaphore()
    for step in range(1, n_gx * n_q):
        peer = lax.rem(row_id * n_q + col_id + step, n_gx * n_q)
        pl.semaphore_signal(
            barrier, inc=1, device_id=device(peer // n_q, lax.rem(peer, n_q)), device_id_type=MESH_ID
        )
    own_w = pltpu.make_async_copy(w_ref, w_all.at[:, :, pl.ds(gz_id * half, half), :], copy_sem.at[0])
    own_w.start()
    pl.semaphore_wait(barrier, n_gx * n_q - 1)

    def push(src, dst, send_sem, recv_sem, to):
        return pltpu.make_async_remote_copy(
            src_ref=src, dst_ref=dst, send_sem=send_sem, recv_sem=recv_sem,
            device_id=to, device_id_type=MESH_ID,
        )

    mate = {"gz": other}
    swaps = [push(x_ref.at[other], x_all.at[gz_id], s_sem.at[0], x_sem.at[0], mate),
             push(g_ref, g_in, s_sem.at[1], x_sem.at[1], mate)]
    for u in range(2):
        swaps.append(
            push(w_ref.at[u], w_all.at[u, :, pl.ds(gz_id * half, half), :], s_sem.at[2 + u], x_sem.at[2 + u], mate)
        )
    for swap in swaps:
        swap.start()
    x_all[gz_id] = x_ref[gz_id]
    mask = m_ref[...]
    own_w.wait()
    swaps[0].wait()
    swaps[1].wait()
    gains = g_ref[...] + g_in[...]
    current = jnp.transpose(x_all[...].reshape(2 * half, side * side), (1, 0))

    for u in range(2):
        swaps[2 + u].wait()
        normed = channel_norm(current, gains[u : u + 1])
        weights = w_all[u, 0:5].reshape(5 * 2 * half, 2 * half)
        projected = rows_dot(normed, weights)
        part = [projected[:, p * 2 * half : (p + 1) * 2 * half] for p in range(5)]
        right = jax.nn.sigmoid(part[2]) * part[3] * mask
        left = jax.nn.sigmoid(part[0]) * part[1] * mask
        if u == 0:
            turn_a[...] = right
            for k in range(side):
                turn_b[pl.ds(k * side, side), :] = turn_a[pl.ds(k, side, stride=side), :]
            right = turn_b[...]
        r_send[u] = right.astype(jnp.bfloat16)
        l_send[u] = left.astype(jnp.bfloat16)
        gate = jax.nn.sigmoid(part[4])
        if u == 0:
            block = col_id
            wide_src, wide_dst = r_send.at[u], r_got.at[u, block]
            wide_to = [device(t, row_id) for t in range(n_gx)]
            wide_self = [on_diag & (row_id == t) for t in range(n_gx)]
            wide_sems = (rs_sem, rr_sem)
            near_src, near_dst = l_send.at[u], l_got.at[u, block]
            near_sems = (ls_sem, lr_sem)
            near_to = [device(row_id, lax.rem(col_id + t, n_q)) for t in range(1, n_q)]
        else:
            block = row_id
            wide_src, wide_dst = l_send.at[u], l_got.at[u, block]
            wide_to = [device(col_id, t) for t in range(n_q)]
            wide_self = [on_diag & (col_id == t) for t in range(n_q)]
            wide_sems = (ls_sem, lr_sem)
            near_src, near_dst = r_send.at[u], r_got.at[u, block]
            near_sems = (rs_sem, rr_sem)
            near_to = [device(lax.rem(row_id + t, n_gx), col_id) for t in range(1, n_gx)]
        sent = []
        for t, to in enumerate(wide_to):
            copy = push(wide_src, wide_dst, wide_sems[0].at[u, t], wide_sems[1].at[u, block], to)
            guard = jnp.logical_not(wide_self[t])
            pl.when(guard)(copy.start)
            sent.append((guard, copy))
        for t, to in enumerate(near_to):
            copy = push(near_src, near_dst, near_sems[0].at[u, t], near_sems[1].at[u, block], to)
            copy.start()
            sent.append((None, copy))

        totals = tuple(jnp.zeros((side, 2 * half), jnp.float32) for _ in range(side))
        steps = n_q if u == 0 else n_gx
        for t in range(steps):
            slot = lax.rem(block + t, steps)
            l_in = push(l_send.at[u], l_got.at[u, slot], ls_sem.at[u, 0], lr_sem.at[u, slot], mate)
            r_in = push(r_send.at[u], r_got.at[u, slot], rs_sem.at[u, 0], rr_sem.at[u, slot], mate)
            wide_in, near_in = (r_in, l_in) if u == 0 else (l_in, r_in)
            wide_got, near_got = (r_got, l_got) if u == 0 else (l_got, r_got)
            wide_mine, near_mine = (r_send, l_send) if u == 0 else (l_send, r_send)
            if t == 0:
                near_got[u, slot] = near_mine[u]

                @pl.when(on_diag)
                def _():
                    wide_got[u, slot] = wide_mine[u]

                pl.when(jnp.logical_not(on_diag))(wide_in.wait_recv)
            else:
                near_in.wait_recv()
                wide_in.wait_recv()
            l_wide[...] = l_got[u, slot].astype(jnp.float32)
            r_wide[...] = r_got[u, slot].astype(jnp.float32)
            fresh = list(totals)
            for k in range(side):
                right_k = r_wide[pl.ds(k * side, side), :]
                for i in range(side):
                    at = i * side + k if u == 0 else k * side + i
                    fresh[i] = fresh[i] + l_wide[pl.ds(at, 1), :] * right_k
            totals = tuple(fresh)
        for i in range(side):
            turn_a[pl.ds(i * side, side), :] = totals[i]
        tri_normed = channel_norm(turn_a[...], gains[2 + u : 3 + u])
        current = current + gate * rows_dot(tri_normed, w_all[u, 5])
        for guard, copy in sent:
            if guard is None:
                copy.wait_send()
            else:
                pl.when(guard)(copy.wait_send)

    z_t[...] = jnp.transpose(current, (1, 0)).reshape(2, half, side * side)
    back = push(z_t.at[other], o_ref.at[gz_id], s_sem.at[4], x_sem.at[4], mate)
    back.start()
    o_ref[gz_id] = z_t[gz_id]
    back.wait()


def fused_device(
    sizes, pair, residue_mask, norm_in_gain, proj_weight, gate_weight, norm_out_gain, out_weight
):
    n_gx, n_gy, n_gz, side = sizes
    half = pair.shape[0]
    full = 2 * half
    pairs = side * side
    n_q = n_gy * n_gz
    gz_id = lax.axis_index("gz")
    row_start = lax.axis_index("gx") * side
    col_start = (lax.axis_index("gy") * n_gz + gz_id) * side
    row_flags = lax.dynamic_slice_in_dim(residue_mask, row_start, side).astype(jnp.float32)
    col_flags = lax.dynamic_slice_in_dim(residue_mask, col_start, side).astype(jnp.float32)
    mask = (row_flags[:, None] * col_flags[None, :]).reshape(pairs, 1)
    x = jnp.transpose(pair.reshape(half, side, n_gz, side), (2, 0, 1, 3)).reshape(n_gz, half, pairs)
    w = jnp.concatenate([proj_weight, gate_weight[:, None], out_weight[:, None]], axis=1)
    w = jnp.transpose(w, (0, 1, 3, 2))
    g = lax.dynamic_update_slice(
        jnp.zeros((8, full), jnp.float32),
        jnp.concatenate([norm_in_gain, norm_out_gain], axis=0),
        (0, gz_id * half),
    )
    vmem = pl.BlockSpec(memory_space=pltpu.VMEM)
    dma = pltpu.SemaphoreType.DMA
    blocks = pltpu.VMEM((2, n_q, pairs, full), jnp.bfloat16)
    out = pl.pallas_call(
        functools.partial(fused_kernel, sizes),
        out_shape=jax.ShapeDtypeStruct((n_gz, half, pairs), jnp.float32),
        in_specs=[vmem] * 4,
        out_specs=vmem,
        scratch_shapes=[
            pltpu.VMEM((n_gz, half, pairs), jnp.float32),
            pltpu.VMEM((2, 6, full, full), jnp.bfloat16),
            pltpu.VMEM((8, full), jnp.float32),
            pltpu.VMEM((2, pairs, full), jnp.bfloat16),
            pltpu.VMEM((2, pairs, full), jnp.bfloat16),
            blocks,
            blocks,
            pltpu.VMEM((pairs, full), jnp.float32),
            pltpu.VMEM((pairs, full), jnp.float32),
            pltpu.VMEM((pairs, full), jnp.float32),
            pltpu.VMEM((pairs, full), jnp.float32),
            pltpu.VMEM((n_gz, half, pairs), jnp.float32),
            dma((5,)), dma((5,)),
            dma((2, n_q)), dma((2, n_q)), dma((2, n_q)), dma((2, n_q)),
            dma((1,)),
        ],
        compiler_params=pltpu.CompilerParams(collective_id=0, has_side_effects=True),
    )(x, w, g, mask)
    out = jnp.transpose(out.reshape(n_gz, half, side, side), (1, 2, 0, 3))
    return out.reshape(half, side, n_gz * side)


def solution(mesh):
    n_gx, n_gy, n_gz = (mesh.shape[name] for name in ("gx", "gy", "gz"))

    def step(pair, *rest):
        _, rows, cols = pair.shape
        square = n_gz == 2 and n_gx == n_gy * n_gz and cols == n_gz * rows
        if square:
            return fused_device((n_gx, n_gy, n_gz, rows), pair, *rest)
        return per_device(pair, *rest)

    return jax.shard_map(
        step,
        mesh=mesh,
        in_specs=(
            P(("groups", "gz"), "gx", "gy"),
            P("groups"),
            P(None, "gz"),
            P(None, None, None, "gz"),
            P(None, None, "gz"),
            P(None, "gz"),
            P(None, None, "gz"),
        ),
        out_specs=P(("groups", "gz"), "gx", "gy"),
        check_vma=False,
    )
```

```python
import functools

import jax
import jax.numpy as jnp
from jax import lax
from jax.experimental import pallas as pl
from jax.experimental.pallas import tpu as pltpu
from jax.sharding import PartitionSpec as P

EPSILON = 1e-05


def layer_norm_gathered(values, gain_part):
    full_values, full_gain = (
        lax.all_gather(values, "gz", axis=0, tiled=True),
        lax.all_gather(gain_part, "gz", axis=0, tiled=True),
    )
    mean_val = jnp.mean(full_values, axis=0)
    centred = full_values - mean_val
    spread = jnp.mean(centred * centred, axis=0)
    result = (centred * lax.rsqrt(spread + EPSILON) * full_gain[:, None, None]).astype(jnp.bfloat16)
    return result


def transpose_tile(pair_tile):
    depth_dim, tile_rows, tile_cols = pair_tile.shape
    across = lax.axis_size("gy")
    down_size = lax.axis_size("gx")
    quarter = tile_rows // across
    spread_rows = lax.all_to_all(pair_tile, "gy", split_axis=1, concat_axis=2, tiled=True)
    blocks = spread_rows.reshape(depth_dim, quarter, down_size, tile_rows)
    blocks = jnp.transpose(blocks, (0, 3, 2, 1))[:, :, :, None, :]
    moved_back = lax.all_to_all(
        lax.all_to_all(blocks, "gx", split_axis=2, concat_axis=2, tiled=True),
        "gy",
        split_axis=2,
        concat_axis=3,
        tiled=True,
    )
    return moved_back.reshape(depth_dim, tile_rows, tile_cols)


def fold_panels(left_tile, right_tile):
    left_panel = lax.all_gather(left_tile, "gy", axis=2, tiled=True)
    return jnp.einsum(
        "hik,hkj->hij",
        left_panel,
        lax.all_gather(right_tile, "gx", axis=1, tiled=True),
        preferred_element_type=jnp.float32,
    )


def per_device(
    pair, residue_mask, norm_in_gain, proj_weight, gate_weight, norm_out_gain, out_weight
):
    tile_rows = pair.shape[1]
    tile_cols = pair.shape[2]
    row_start = lax.axis_index("gx") * tile_rows
    col_start = lax.axis_index("gy") * tile_cols
    row_flags = lax.dynamic_slice_in_dim(residue_mask, row_start, tile_rows).astype(jnp.float32)
    col_flags = lax.dynamic_slice_in_dim(residue_mask, col_start, tile_cols).astype(jnp.float32)
    pair_mask = row_flags[:, None] * col_flags[None, :]
    current = pair
    for update in range(2):
        normed = layer_norm_gathered(current, norm_in_gain[update])
        projected = jnp.einsum(
            "cij,pch->phij", normed, proj_weight[update], preferred_element_type=jnp.float32
        )
        left_tile = (jax.nn.sigmoid(projected[0]) * projected[1] * pair_mask).astype(jnp.bfloat16)
        right_tile = (jax.nn.sigmoid(projected[2]) * projected[3] * pair_mask).astype(jnp.bfloat16)
        gate_values = jax.nn.sigmoid(
            jnp.einsum(
                "cij,cd->dij", normed, gate_weight[update], preferred_element_type=jnp.float32
            )
        )
        if update == 0:
            triangle = fold_panels(left_tile, transpose_tile(right_tile))
        else:
            triangle = fold_panels(transpose_tile(left_tile), right_tile)
        tri_normed = layer_norm_gathered(triangle, norm_out_gain[update])
        current = current + gate_values * jnp.einsum(
            "hij,hd->dij", tri_normed, out_weight[update], preferred_element_type=jnp.float32
        )
    return current


MESH_ID = pl.DeviceIdType.MESH


def channel_norm(values, gain_row):
    mean_val = jnp.mean(values, axis=1, keepdims=True)
    centred = values - mean_val
    spread = jnp.mean(centred * centred, axis=1, keepdims=True)
    return (centred * lax.rsqrt(spread + EPSILON) * gain_row).astype(jnp.bfloat16)


def rows_dot(rows, weight_t):
    return lax.dot_general(
        rows, weight_t, (((1,), (1,)), ((), ())), preferred_element_type=jnp.float32
    )


def fused_kernel(
    sizes, x_ref, mask_ref, gin_ref, proj_ref, gate_ref, gout_ref, outw_ref, o_ref,
    x_in, x_out, x_got, p_all, g_all, d_all, gain_own, gain_got, l_send, r_send, l_got, r_got,
    l_wide, r_wide, turn_a, turn_b, z_out, z_got,
    s_sem, x_sem, ls_sem, rs_sem, lr_sem, rr_sem, copy_sem,
):
    n_gx, n_gy, n_gz, side = sizes
    n_q = n_gy * n_gz
    row_id, gy_id, gz_id = lax.axis_index("gx"), lax.axis_index("gy"), lax.axis_index("gz")
    col_id = gy_id * n_gz + gz_id
    other = 1 - gz_id
    half = x_ref.shape[2]
    full = 2 * half
    pairs = side * side
    on_diag = row_id == col_id
    first = gz_id == 0
    own_rows = pl.ds(pl.multiple_of(gz_id * half, half), half)

    def device(at_row, at_col):
        return {"gx": at_row, "gy": at_col // n_gz, "gz": lax.rem(at_col, n_gz)}

    def push(src, dst, send_sem, recv_sem, to):
        return pltpu.make_async_remote_copy(
            src_ref=src, dst_ref=dst, send_sem=send_sem, recv_sem=recv_sem,
            device_id=to, device_id_type=MESH_ID,
        )

    loads = [
        pltpu.make_async_copy(src, dst, copy_sem.at[n])
        for n, (src, dst) in enumerate((
            (x_ref, x_in),
            (proj_ref.at[0], p_all.at[0, :, own_rows, :]),
            (gate_ref.at[0], g_all.at[0, own_rows, :]),
            (outw_ref.at[0], d_all.at[0, own_rows, :]),
            (proj_ref.at[1], p_all.at[1, :, own_rows, :]),
            (gate_ref.at[1], g_all.at[1, own_rows, :]),
            (outw_ref.at[1], d_all.at[1, own_rows, :]),
        ))
    ]
    for load in loads:
        load.start()
    barrier = pltpu.get_barrier_semaphore()
    for step in range(1, n_gx * n_q):
        peer = lax.rem(row_id * n_q + col_id + step, n_gx * n_q)
        pl.semaphore_signal(
            barrier, inc=1, device_id=device(peer // n_q, lax.rem(peer, n_q)), device_id_type=MESH_ID
        )

    low_lanes = lax.broadcasted_iota(jnp.int32, (pairs, full), 1) < half
    low_packed = low_lanes[: pairs // 2]

    def pack(rows):
        return jnp.where(low_packed, rows[: pairs // 2], pltpu.roll(rows[pairs // 2 :], half, 1))

    def unpack(packed):
        return jnp.concatenate([packed, pltpu.roll(packed, half, 1)], axis=0)

    gain_own[...] = jnp.zeros_like(gain_own)
    gain_own[0:2, 0:half] = gin_ref[...]
    gain_own[2:4, 0:half] = gout_ref[...]
    loads[0].wait()
    turn_a[...] = jnp.zeros_like(turn_a)
    turn_b[...] = jnp.zeros_like(turn_b)
    for i in range(side):
        left_cols, right_cols = x_in[i, 0:side, :], x_in[i, side : 2 * side, :]
        turn_a[pl.ds(i * side, side), 0:half] = jnp.where(first, left_cols, right_cols)
        turn_b[pl.ds(i * side, side), 0:half] = jnp.where(first, right_cols, left_cols)
    x_out[...] = pack(turn_b[...])

    n_res = mask_ref.shape[1]
    pair_no = lax.broadcasted_iota(jnp.int32, (pairs, n_res), 0)
    residue = lax.broadcasted_iota(jnp.int32, (pairs, n_res), 1)
    in_row = ((pair_no.astype(jnp.float32) + 0.5) / side).astype(jnp.int32)
    in_col = pair_no - in_row * side
    flags = mask_ref[...].astype(jnp.float32)
    row_flag = jnp.sum(jnp.where(residue == in_row + row_id * side, flags, 0.0), axis=1, keepdims=True)
    col_flag = jnp.sum(jnp.where(residue == in_col + col_id * side, flags, 0.0), axis=1, keepdims=True)
    mask = row_flag * col_flag

    pl.semaphore_wait(barrier, n_gx * n_q - 1)
    mate = {"gz": other}
    swaps = [
        push(src, dst, s_sem.at[n], x_sem.at[n], mate)
        for n, (src, dst) in enumerate((
            (x_out, x_got),
            (gain_own, gain_got),
            (proj_ref.at[0], p_all.at[0, :, own_rows, :]),
            (gate_ref.at[0], g_all.at[0, own_rows, :]),
            (outw_ref.at[0], d_all.at[0, own_rows, :]),
            (proj_ref.at[1], p_all.at[1, :, own_rows, :]),
            (gate_ref.at[1], g_all.at[1, own_rows, :]),
            (outw_ref.at[1], d_all.at[1, own_rows, :]),
        ))
    ]
    for swap in swaps:
        swap.start()
    swaps[0].wait()
    swaps[1].wait()

    def merge(mine, theirs, lanes):
        low, high = jnp.where(first, mine, theirs), jnp.where(first, theirs, mine)
        return jnp.where(lanes, low, pltpu.roll(high, half, 1))

    gains = merge(gain_own[...], gain_got[...], low_lanes[0:8])
    current = merge(turn_a[...], unpack(x_got[...]), low_lanes)

    for u in range(2):
        normed = channel_norm(current, gains[u : u + 1])
        loads[1 + 3 * u].wait()
        swaps[2 + 3 * u].wait()
        projected = rows_dot(normed, p_all[u].reshape(4 * full, full))
        part = [projected[:, p * full : (p + 1) * full] for p in range(4)]
        right = jax.nn.sigmoid(part[2]) * part[3] * mask
        left = jax.nn.sigmoid(part[0]) * part[1] * mask
        if u == 0:
            turn_a[...] = right
            for k in range(side):
                turn_b[pl.ds(k * side, side), :] = turn_a[pl.ds(k, side, stride=side), :]
            right = turn_b[...]
        r_send[u] = right.astype(jnp.bfloat16)
        l_send[u] = left.astype(jnp.bfloat16)
        if u == 0:
            block = col_id
            wide_src, wide_dst = r_send.at[u], r_got.at[u, block]
            wide_to = [device(t, row_id) for t in range(n_gx)]
            wide_self = [on_diag & (row_id == t) for t in range(n_gx)]
            wide_sems = (rs_sem, rr_sem)
            near_src, near_dst = l_send.at[u], l_got.at[u, block]
            near_sems = (ls_sem, lr_sem)
            near_to = [device(row_id, lax.rem(col_id + t, n_q)) for t in range(1, n_q)]
        else:
            block = row_id
            wide_src, wide_dst = l_send.at[u], l_got.at[u, block]
            wide_to = [device(col_id, t) for t in range(n_q)]
            wide_self = [on_diag & (col_id == t) for t in range(n_q)]
            wide_sems = (ls_sem, lr_sem)
            near_src, near_dst = r_send.at[u], r_got.at[u, block]
            near_sems = (rs_sem, rr_sem)
            near_to = [device(lax.rem(row_id + t, n_gx), col_id) for t in range(1, n_gx)]
        sent = []
        for t, to in enumerate(wide_to):
            copy = push(wide_src, wide_dst, wide_sems[0].at[u, t], wide_sems[1].at[u, block], to)
            guard = jnp.logical_not(wide_self[t])
            pl.when(guard)(copy.start)
            sent.append((guard, copy))
        for t, to in enumerate(near_to):
            copy = push(near_src, near_dst, near_sems[0].at[u, t], near_sems[1].at[u, block], to)
            copy.start()
            sent.append((None, copy))

        for n in (1, 2):
            loads[1 + 3 * u + n].wait()
            swaps[2 + 3 * u + n].wait()
        gate = jax.nn.sigmoid(rows_dot(normed, g_all[u]))
        totals = tuple(jnp.zeros((side, full), jnp.float32) for _ in range(side))
        steps = n_q if u == 0 else n_gx
        for t in range(steps):
            slot = lax.rem(block + t, steps)
            l_in = push(l_send.at[u], l_got.at[u, slot], ls_sem.at[u, 0], lr_sem.at[u, slot], mate)
            r_in = push(r_send.at[u], r_got.at[u, slot], rs_sem.at[u, 0], rr_sem.at[u, slot], mate)
            wide_in, near_in = (r_in, l_in) if u == 0 else (l_in, r_in)
            wide_got, near_got = (r_got, l_got) if u == 0 else (l_got, r_got)
            wide_mine, near_mine = (r_send, l_send) if u == 0 else (l_send, r_send)
            if t == 0:
                near_got[u, slot] = near_mine[u]

                @pl.when(on_diag)
                def _():
                    wide_got[u, slot] = wide_mine[u]

                pl.when(jnp.logical_not(on_diag))(wide_in.wait_recv)
            else:
                near_in.wait_recv()
                wide_in.wait_recv()
            l_wide[...] = l_got[u, slot].astype(jnp.float32)
            r_wide[...] = r_got[u, slot].astype(jnp.float32)
            fresh = list(totals)
            for k in range(side):
                right_k = r_wide[pl.ds(k * side, side), :]
                for i in range(side):
                    at = i * side + k if u == 0 else k * side + i
                    fresh[i] = fresh[i] + l_wide[pl.ds(at, 1), :] * right_k
            totals = tuple(fresh)
        for i in range(side):
            turn_a[pl.ds(i * side, side), :] = totals[i]
        tri_normed = channel_norm(turn_a[...], gains[2 + u : 3 + u])
        current = current + gate * rows_dot(tri_normed, d_all[u])
        for guard, copy in sent:
            if guard is None:
                copy.wait_send()
            else:
                pl.when(guard)(copy.wait_send)

    turned = pltpu.roll(current, half, 1)
    z_out[...] = pack(jnp.where(first, turned, current))
    back = push(z_out, z_got, s_sem.at[8], x_sem.at[8], mate)
    back.start()
    turn_a[...] = jnp.where(first, current, turned)
    back.wait()
    turn_b[...] = unpack(z_got[...])
    for i in range(side):
        mine, theirs = turn_a[pl.ds(i * side, side), 0:half], turn_b[pl.ds(i * side, side), 0:half]
        o_ref[i, 0:side, :] = jnp.where(first, mine, theirs)
        o_ref[i, side : 2 * side, :] = jnp.where(first, theirs, mine)


def fused_device(
    sizes, pair, residue_mask, norm_in_gain, proj_weight, gate_weight, norm_out_gain, out_weight
):
    n_gx, n_gy, n_gz, side = sizes
    half = pair.shape[0]
    full = 2 * half
    pairs = side * side
    n_q = n_gy * n_gz
    vmem = pl.BlockSpec(memory_space=pltpu.VMEM)
    hbm = pl.BlockSpec(memory_space=pl.ANY)
    dma = pltpu.SemaphoreType.DMA
    blocks = pltpu.VMEM((2, n_q, pairs, full), jnp.bfloat16)
    block = pltpu.VMEM((pairs, full), jnp.float32)
    packed = pltpu.VMEM((pairs // 2, full), jnp.float32)
    out = pl.pallas_call(
        functools.partial(fused_kernel, sizes),
        out_shape=jax.ShapeDtypeStruct((side, n_gz * side, half), jnp.float32),
        in_specs=[hbm, vmem, vmem, hbm, hbm, vmem, hbm],
        out_specs=vmem,
        scratch_shapes=[
            pltpu.VMEM((side, n_gz * side, half), jnp.float32),
            packed,
            packed,
            pltpu.VMEM((2, 4, full, full), jnp.bfloat16),
            pltpu.VMEM((2, full, full), jnp.bfloat16),
            pltpu.VMEM((2, full, full), jnp.bfloat16),
            pltpu.VMEM((8, full), jnp.float32),
            pltpu.VMEM((8, full), jnp.float32),
            pltpu.VMEM((2, pairs, full), jnp.bfloat16),
            pltpu.VMEM((2, pairs, full), jnp.bfloat16),
            blocks, blocks,
            block, block, block, block,
            packed, packed,
            dma((9,)), dma((9,)),
            dma((2, n_q)), dma((2, n_q)), dma((2, n_q)), dma((2, n_q)),
            dma((7,)),
        ],
        compiler_params=pltpu.CompilerParams(collective_id=0, has_side_effects=True),
    )(
        jnp.transpose(pair, (1, 2, 0)),
        residue_mask[None, :],
        norm_in_gain,
        jnp.transpose(proj_weight, (0, 1, 3, 2)),
        jnp.transpose(gate_weight, (0, 2, 1)),
        norm_out_gain,
        jnp.transpose(out_weight, (0, 2, 1)),
    )
    return jnp.transpose(out, (2, 0, 1))


def solution(mesh):
    n_gx, n_gy, n_gz = (mesh.shape[name] for name in ("gx", "gy", "gz"))

    def step(pair, *rest):
        _, rows, cols = pair.shape
        square = n_gz == 2 and n_gx == n_gy * n_gz and cols == n_gz * rows and rows % 4 == 0
        if square:
            return fused_device((n_gx, n_gy, n_gz, rows), pair, *rest)
        return per_device(pair, *rest)

    return jax.shard_map(
        step,
        mesh=mesh,
        in_specs=(
            P(("groups", "gz"), "gx", "gy"),
            P("groups"),
            P(None, "gz"),
            P(None, None, None, "gz"),
            P(None, None, "gz"),
            P(None, "gz"),
            P(None, None, "gz"),
        ),
        out_specs=P(("groups", "gz"), "gx", "gy"),
        check_vma=False,
    )
```

```python
import functools

import jax
import jax.numpy as jnp
from jax import lax
from jax.experimental import pallas as pl
from jax.experimental.pallas import tpu as pltpu
from jax.sharding import PartitionSpec as P

EPSILON = 1e-05


def layer_norm_gathered(values, gain_part):
    full_values, full_gain = (
        lax.all_gather(values, "gz", axis=0, tiled=True),
        lax.all_gather(gain_part, "gz", axis=0, tiled=True),
    )
    mean_val = jnp.mean(full_values, axis=0)
    centred = full_values - mean_val
    spread = jnp.mean(centred * centred, axis=0)
    result = (centred * lax.rsqrt(spread + EPSILON) * full_gain[:, None, None]).astype(jnp.bfloat16)
    return result


def transpose_tile(pair_tile):
    depth_dim, tile_rows, tile_cols = pair_tile.shape
    across = lax.axis_size("gy")
    down_size = lax.axis_size("gx")
    quarter = tile_rows // across
    spread_rows = lax.all_to_all(pair_tile, "gy", split_axis=1, concat_axis=2, tiled=True)
    blocks = spread_rows.reshape(depth_dim, quarter, down_size, tile_rows)
    blocks = jnp.transpose(blocks, (0, 3, 2, 1))[:, :, :, None, :]
    moved_back = lax.all_to_all(
        lax.all_to_all(blocks, "gx", split_axis=2, concat_axis=2, tiled=True),
        "gy",
        split_axis=2,
        concat_axis=3,
        tiled=True,
    )
    return moved_back.reshape(depth_dim, tile_rows, tile_cols)


def fold_panels(left_tile, right_tile):
    left_panel = lax.all_gather(left_tile, "gy", axis=2, tiled=True)
    return jnp.einsum(
        "hik,hkj->hij",
        left_panel,
        lax.all_gather(right_tile, "gx", axis=1, tiled=True),
        preferred_element_type=jnp.float32,
    )


def per_device(
    pair, residue_mask, norm_in_gain, proj_weight, gate_weight, norm_out_gain, out_weight
):
    tile_rows = pair.shape[1]
    tile_cols = pair.shape[2]
    row_start = lax.axis_index("gx") * tile_rows
    col_start = lax.axis_index("gy") * tile_cols
    row_flags = lax.dynamic_slice_in_dim(residue_mask, row_start, tile_rows).astype(jnp.float32)
    col_flags = lax.dynamic_slice_in_dim(residue_mask, col_start, tile_cols).astype(jnp.float32)
    pair_mask = row_flags[:, None] * col_flags[None, :]
    current = pair
    for update in range(2):
        normed = layer_norm_gathered(current, norm_in_gain[update])
        projected = jnp.einsum(
            "cij,pch->phij", normed, proj_weight[update], preferred_element_type=jnp.float32
        )
        left_tile = (jax.nn.sigmoid(projected[0]) * projected[1] * pair_mask).astype(jnp.bfloat16)
        right_tile = (jax.nn.sigmoid(projected[2]) * projected[3] * pair_mask).astype(jnp.bfloat16)
        gate_values = jax.nn.sigmoid(
            jnp.einsum(
                "cij,cd->dij", normed, gate_weight[update], preferred_element_type=jnp.float32
            )
        )
        if update == 0:
            triangle = fold_panels(left_tile, transpose_tile(right_tile))
        else:
            triangle = fold_panels(transpose_tile(left_tile), right_tile)
        tri_normed = layer_norm_gathered(triangle, norm_out_gain[update])
        current = current + gate_values * jnp.einsum(
            "hij,hd->dij", tri_normed, out_weight[update], preferred_element_type=jnp.float32
        )
    return current


MESH_ID = pl.DeviceIdType.MESH


def channel_norm(values, gain_row):
    mean_val = jnp.mean(values, axis=1, keepdims=True)
    centred = values - mean_val
    spread = jnp.mean(centred * centred, axis=1, keepdims=True)
    return (centred * lax.rsqrt(spread + EPSILON) * gain_row).astype(jnp.bfloat16)


def rows_dot(rows, weight_t):
    return lax.dot_general(
        rows, weight_t, (((1,), (1,)), ((), ())), preferred_element_type=jnp.float32
    )


def fused_kernel(
    sizes, x_ref, mask_ref, gin_ref, proj_ref, gate_ref, gout_ref, outw_ref, o_ref,
    x_in, x_out, x_got, p_all, g_all, d_all, gain_own, gain_got, l_send, r_send, part_send, l_got, r_got,
    l_wide, r_wide, turn_a, turn_b, z_out, z_got,
    s_sem, x_sem, ls_sem, rs_sem, lr_sem, rr_sem, copy_sem,
):
    n_gx, n_gy, n_gz, side = sizes
    n_q = n_gy * n_gz
    row_id, gy_id, gz_id = lax.axis_index("gx"), lax.axis_index("gy"), lax.axis_index("gz")
    col_id = gy_id * n_gz + gz_id
    other = 1 - gz_id
    half = x_ref.shape[2]
    full = 2 * half
    pairs = side * side
    on_diag = row_id == col_id
    first = gz_id == 0
    own_rows = pl.ds(pl.multiple_of(gz_id * half, half), half)

    def device(at_row, at_col):
        return {"gx": at_row, "gy": at_col // n_gz, "gz": lax.rem(at_col, n_gz)}

    def push(src, dst, send_sem, recv_sem, to):
        return pltpu.make_async_remote_copy(
            src_ref=src, dst_ref=dst, send_sem=send_sem, recv_sem=recv_sem,
            device_id=to, device_id_type=MESH_ID,
        )

    loads = [
        pltpu.make_async_copy(src, dst, copy_sem.at[n])
        for n, (src, dst) in enumerate((
            (x_ref, x_in),
            (proj_ref.at[0], p_all.at[0, :, own_rows, :]),
            (gate_ref.at[0], g_all.at[0, own_rows, :]),
            (outw_ref.at[0], d_all.at[0, own_rows, :]),
            (proj_ref.at[1], p_all.at[1, :, own_rows, :]),
            (gate_ref.at[1], g_all.at[1, own_rows, :]),
            (outw_ref.at[1], d_all.at[1, own_rows, :]),
        ))
    ]
    for load in loads:
        load.start()
    barrier = pltpu.get_barrier_semaphore()
    for step in range(1, n_gx * n_q):
        peer = lax.rem(row_id * n_q + col_id + step, n_gx * n_q)
        pl.semaphore_signal(
            barrier, inc=1, device_id=device(peer // n_q, lax.rem(peer, n_q)), device_id_type=MESH_ID
        )

    low_lanes = lax.broadcasted_iota(jnp.int32, (pairs, full), 1) < half
    low_packed = low_lanes[: pairs // 2]

    def pack(rows):
        return jnp.where(low_packed, rows[: pairs // 2], pltpu.roll(rows[pairs // 2 :], half, 1))

    def unpack(packed):
        return jnp.concatenate([packed, pltpu.roll(packed, half, 1)], axis=0)

    gain_own[...] = jnp.zeros_like(gain_own)
    gain_own[0:2, 0:half] = gin_ref[...]
    gain_own[2:4, 0:half] = gout_ref[...]
    loads[0].wait()
    turn_a[...] = jnp.zeros_like(turn_a)
    turn_b[...] = jnp.zeros_like(turn_b)
    for i in range(side):
        left_cols, right_cols = x_in[i, 0:side, :], x_in[i, side : 2 * side, :]
        turn_a[pl.ds(i * side, side), 0:half] = jnp.where(first, left_cols, right_cols)
        turn_b[pl.ds(i * side, side), 0:half] = jnp.where(first, right_cols, left_cols)
    x_out[...] = pack(turn_b[...])

    n_res = mask_ref.shape[1]
    pair_no = lax.broadcasted_iota(jnp.int32, (pairs, n_res), 0)
    residue = lax.broadcasted_iota(jnp.int32, (pairs, n_res), 1)
    in_row = ((pair_no.astype(jnp.float32) + 0.5) / side).astype(jnp.int32)
    in_col = pair_no - in_row * side
    flags = mask_ref[...].astype(jnp.float32)
    row_flag = jnp.sum(jnp.where(residue == in_row + row_id * side, flags, 0.0), axis=1, keepdims=True)
    col_flag = jnp.sum(jnp.where(residue == in_col + col_id * side, flags, 0.0), axis=1, keepdims=True)
    mask = row_flag * col_flag

    pl.semaphore_wait(barrier, n_gx * n_q - 1)
    mate = {"gz": other}
    swaps = [
        push(src, dst, s_sem.at[n], x_sem.at[n], mate)
        for n, (src, dst) in enumerate((
            (x_out, x_got),
            (gain_own, gain_got),
            (proj_ref.at[0], p_all.at[0, :, own_rows, :]),
            (gate_ref.at[0], g_all.at[0, own_rows, :]),
            (outw_ref.at[0], d_all.at[0, own_rows, :]),
            (proj_ref.at[1], p_all.at[1, :, own_rows, :]),
            (gate_ref.at[1], g_all.at[1, own_rows, :]),
            (outw_ref.at[1], d_all.at[1, own_rows, :]),
        ))
    ]
    for swap in swaps:
        swap.start()
    swaps[0].wait()
    swaps[1].wait()

    def merge(mine, theirs, lanes):
        low, high = jnp.where(first, mine, theirs), jnp.where(first, theirs, mine)
        return jnp.where(lanes, low, pltpu.roll(high, half, 1))

    gains = merge(gain_own[...], gain_got[...], low_lanes[0:8])
    current = merge(turn_a[...], unpack(x_got[...]), low_lanes)

    for u in range(2):
        normed = channel_norm(current, gains[u : u + 1])
        loads[1 + 3 * u].wait()
        swaps[2 + 3 * u].wait()
        def gated(side_no):
            projected = rows_dot(normed, p_all[u, 2 * side_no : 2 * side_no + 2].reshape(2 * full, full))
            return jax.nn.sigmoid(projected[:, :full]) * projected[:, full:] * mask

        def side_sends(what, targets):
            src, dst, send_sems, recv_sems = what
            for t, (to, guard) in enumerate(targets):
                copy = push(src, dst, send_sems.at[u, t], recv_sems, to)
                if guard is None:
                    copy.start()
                else:
                    pl.when(guard)(copy.start)
                sent.append((guard, copy))

        def block_product(totals, left_row):
            fresh = list(totals)
            for k in range(side):
                right_k = r_wide[pl.ds(k * side, side), :]
                for i in range(side):
                    fresh[i] = fresh[i] + l_wide[pl.ds(left_row(k, i), 1), :] * right_k
            return fresh

        def late_weights():
            for n in (1, 2):
                loads[1 + 3 * u + n].wait()
                swaps[2 + 3 * u + n].wait()
            return jax.nn.sigmoid(rows_dot(normed, g_all[u]))

        sent = []
        plane = [
            lax.rem(gy_id + t // n_gz, n_gy) * n_gz + lax.rem(gz_id + t, n_gz) for t in range(n_q)
        ]
        in_plane = [(device(row_id, at), None) for at in plane[:0:-1]]
        zeros = [jnp.zeros((side, full), jnp.float32) for _ in range(side)]
        if u == 0:
            right_end = row_id >= n_gx // 2
            far_rows = [jnp.where(right_end, t, n_gx - 1 - t) for t in range(n_gx)]
            turn_a[...] = gated(1)
            for k in range(side):
                turn_b[pl.ds(k * side, side), :] = turn_a[pl.ds(k, side, stride=side), :]
            r_send[...] = turn_b[...].astype(jnp.bfloat16)
            side_sends(
                (r_send, r_got.at[u, col_id], rs_sem, rr_sem.at[u, col_id]),
                [(device(t, row_id), jnp.logical_not(on_diag & (row_id == t))) for t in far_rows],
            )
            l_send[u] = gated(0).astype(jnp.bfloat16)
            side_sends((l_send.at[u], l_got.at[u, col_id], ls_sem, lr_sem.at[u, col_id]), in_plane)
            gate = late_weights()
            totals = zeros
            for t, slot in enumerate(plane):
                l_in = push(l_send.at[u], l_got.at[u, slot], ls_sem.at[u, 0], lr_sem.at[u, slot], mate)
                r_in = push(r_send, r_got.at[u, slot], rs_sem.at[u, 0], rr_sem.at[u, slot], mate)
                if t == 0:
                    l_wide[...] = l_send[u].astype(jnp.float32)

                    @pl.when(on_diag)
                    def _():
                        r_got[u, slot] = r_send[...]

                    pl.when(jnp.logical_not(on_diag))(r_in.wait_recv)
                else:
                    l_in.wait_recv()
                    r_in.wait_recv()
                    l_wide[...] = l_got[u, slot].astype(jnp.float32)
                r_wide[...] = r_got[u, slot].astype(jnp.float32)
                totals = block_product(totals, lambda k, i: i * side + k)
            for i in range(side):
                turn_a[pl.ds(i * side, side), :] = totals[i]
        else:
            l_send[u] = gated(0).astype(jnp.bfloat16)
            side_sends((l_send.at[u], l_got.at[u, col_id], ls_sem, lr_sem.at[u, col_id]), in_plane)
            r_wide[...] = gated(1).astype(jnp.bfloat16).astype(jnp.float32)
            gate = late_weights()
            for t, slot in enumerate(plane):
                if t == 0:
                    l_wide[...] = l_send[u].astype(jnp.float32)
                else:
                    push(l_send.at[u], l_got.at[u, slot], ls_sem.at[u, 0], lr_sem.at[u, slot], mate).wait_recv()
                    l_wide[...] = l_got[u, slot].astype(jnp.float32)
                totals = block_product(zeros, lambda k, i: k * side + i)
                for i in range(side):
                    turn_b[pl.ds(i * side, side), :] = totals[i]
                part_send[t] = turn_b[...].astype(jnp.bfloat16)

                @pl.when(slot == row_id)
                def _():
                    turn_a[...] = turn_b[...]

                copy = push(
                    part_send.at[t], r_got.at[u, row_id], rs_sem.at[u, t], rr_sem.at[u, row_id],
                    device(slot, col_id),
                )
                pl.when(slot != row_id)(copy.start)
                sent.append((slot != row_id, copy))
            for t in range(1, n_gx):
                slot = lax.rem(row_id + t, n_gx)
                push(part_send.at[0], r_got.at[u, slot], rs_sem.at[u, 0], rr_sem.at[u, slot], mate).wait_recv()
                turn_a[...] += r_got[u, slot].astype(jnp.float32)
        tri_normed = channel_norm(turn_a[...], gains[2 + u : 3 + u])
        current = current + gate * rows_dot(tri_normed, d_all[u])
        for guard, copy in sent:
            if guard is None:
                copy.wait_send()
            else:
                pl.when(guard)(copy.wait_send)

    turned = pltpu.roll(current, half, 1)
    z_out[...] = pack(jnp.where(first, turned, current))
    back = push(z_out, z_got, s_sem.at[8], x_sem.at[8], mate)
    back.start()
    turn_a[...] = jnp.where(first, current, turned)
    back.wait()
    turn_b[...] = unpack(z_got[...])
    for i in range(side):
        mine, theirs = turn_a[pl.ds(i * side, side), 0:half], turn_b[pl.ds(i * side, side), 0:half]
        o_ref[i, 0:side, :] = jnp.where(first, mine, theirs)
        o_ref[i, side : 2 * side, :] = jnp.where(first, theirs, mine)


def fused_device(
    sizes, pair, residue_mask, norm_in_gain, proj_weight, gate_weight, norm_out_gain, out_weight
):
    n_gx, n_gy, n_gz, side = sizes
    half = pair.shape[0]
    full = 2 * half
    pairs = side * side
    n_q = n_gy * n_gz
    vmem = pl.BlockSpec(memory_space=pltpu.VMEM)
    hbm = pl.BlockSpec(memory_space=pl.ANY)
    dma = pltpu.SemaphoreType.DMA
    blocks = pltpu.VMEM((2, n_q, pairs, full), jnp.bfloat16)
    block = pltpu.VMEM((pairs, full), jnp.float32)
    packed = pltpu.VMEM((pairs // 2, full), jnp.float32)
    out = pl.pallas_call(
        functools.partial(fused_kernel, sizes),
        out_shape=jax.ShapeDtypeStruct((side, n_gz * side, half), jnp.float32),
        in_specs=[hbm, vmem, vmem, hbm, hbm, vmem, hbm],
        out_specs=vmem,
        scratch_shapes=[
            pltpu.VMEM((side, n_gz * side, half), jnp.float32),
            packed,
            packed,
            pltpu.VMEM((2, 4, full, full), jnp.bfloat16),
            pltpu.VMEM((2, full, full), jnp.bfloat16),
            pltpu.VMEM((2, full, full), jnp.bfloat16),
            pltpu.VMEM((8, full), jnp.float32),
            pltpu.VMEM((8, full), jnp.float32),
            pltpu.VMEM((2, pairs, full), jnp.bfloat16),
            pltpu.VMEM((pairs, full), jnp.bfloat16),
            pltpu.VMEM((n_q, pairs, full), jnp.bfloat16),
            blocks, blocks,
            block, block, block, block,
            packed, packed,
            dma((9,)), dma((9,)),
            dma((2, n_q)), dma((2, n_q)), dma((2, n_q)), dma((2, n_q)),
            dma((7,)),
        ],
        compiler_params=pltpu.CompilerParams(collective_id=0, has_side_effects=True),
    )(
        jnp.transpose(pair, (1, 2, 0)),
        residue_mask[None, :],
        norm_in_gain,
        jnp.transpose(proj_weight, (0, 1, 3, 2)),
        jnp.transpose(gate_weight, (0, 2, 1)),
        norm_out_gain,
        jnp.transpose(out_weight, (0, 2, 1)),
    )
    return jnp.transpose(out, (2, 0, 1))


def solution(mesh):
    n_gx, n_gy, n_gz = (mesh.shape[name] for name in ("gx", "gy", "gz"))

    def step(pair, *rest):
        _, rows, cols = pair.shape
        square = n_gz == 2 and n_gx == n_gy * n_gz and cols == n_gz * rows and rows % 4 == 0
        if square:
            return fused_device((n_gx, n_gy, n_gz, rows), pair, *rest)
        return per_device(pair, *rest)

    return jax.shard_map(
        step,
        mesh=mesh,
        in_specs=(
            P(("groups", "gz"), "gx", "gy"),
            P("groups"),
            P(None, "gz"),
            P(None, None, None, "gz"),
            P(None, None, "gz"),
            P(None, "gz"),
            P(None, None, "gz"),
        ),
        out_specs=P(("groups", "gz"), "gx", "gy"),
        check_vma=False,
    )
```

```python
import functools

import jax
import jax.numpy as jnp
from jax import lax
from jax.experimental import pallas as pl
from jax.experimental.pallas import tpu as pltpu
from jax.sharding import PartitionSpec as P

EPSILON = 1e-05


def layer_norm_gathered(values, gain_part):
    full_values, full_gain = (
        lax.all_gather(values, "gz", axis=0, tiled=True),
        lax.all_gather(gain_part, "gz", axis=0, tiled=True),
    )
    mean_val = jnp.mean(full_values, axis=0)
    centred = full_values - mean_val
    spread = jnp.mean(centred * centred, axis=0)
    result = (centred * lax.rsqrt(spread + EPSILON) * full_gain[:, None, None]).astype(jnp.bfloat16)
    return result


def transpose_tile(pair_tile):
    depth_dim, tile_rows, tile_cols = pair_tile.shape
    across = lax.axis_size("gy")
    down_size = lax.axis_size("gx")
    quarter = tile_rows // across
    spread_rows = lax.all_to_all(pair_tile, "gy", split_axis=1, concat_axis=2, tiled=True)
    blocks = spread_rows.reshape(depth_dim, quarter, down_size, tile_rows)
    blocks = jnp.transpose(blocks, (0, 3, 2, 1))[:, :, :, None, :]
    moved_back = lax.all_to_all(
        lax.all_to_all(blocks, "gx", split_axis=2, concat_axis=2, tiled=True),
        "gy",
        split_axis=2,
        concat_axis=3,
        tiled=True,
    )
    return moved_back.reshape(depth_dim, tile_rows, tile_cols)


def fold_panels(left_tile, right_tile):
    left_panel = lax.all_gather(left_tile, "gy", axis=2, tiled=True)
    return jnp.einsum(
        "hik,hkj->hij",
        left_panel,
        lax.all_gather(right_tile, "gx", axis=1, tiled=True),
        preferred_element_type=jnp.float32,
    )


def per_device(
    pair, residue_mask, norm_in_gain, proj_weight, gate_weight, norm_out_gain, out_weight
):
    tile_rows = pair.shape[1]
    tile_cols = pair.shape[2]
    row_start = lax.axis_index("gx") * tile_rows
    col_start = lax.axis_index("gy") * tile_cols
    row_flags = lax.dynamic_slice_in_dim(residue_mask, row_start, tile_rows).astype(jnp.float32)
    col_flags = lax.dynamic_slice_in_dim(residue_mask, col_start, tile_cols).astype(jnp.float32)
    pair_mask = row_flags[:, None] * col_flags[None, :]
    current = pair
    for update in range(2):
        normed = layer_norm_gathered(current, norm_in_gain[update])
        projected = jnp.einsum(
            "cij,pch->phij", normed, proj_weight[update], preferred_element_type=jnp.float32
        )
        left_tile = (jax.nn.sigmoid(projected[0]) * projected[1] * pair_mask).astype(jnp.bfloat16)
        right_tile = (jax.nn.sigmoid(projected[2]) * projected[3] * pair_mask).astype(jnp.bfloat16)
        gate_values = jax.nn.sigmoid(
            jnp.einsum(
                "cij,cd->dij", normed, gate_weight[update], preferred_element_type=jnp.float32
            )
        )
        if update == 0:
            triangle = fold_panels(left_tile, transpose_tile(right_tile))
        else:
            triangle = fold_panels(transpose_tile(left_tile), right_tile)
        tri_normed = layer_norm_gathered(triangle, norm_out_gain[update])
        current = current + gate_values * jnp.einsum(
            "hij,hd->dij", tri_normed, out_weight[update], preferred_element_type=jnp.float32
        )
    return current


MESH_ID = pl.DeviceIdType.MESH


def channel_norm(values, gain_row):
    mean_val = jnp.mean(values, axis=1, keepdims=True)
    centred = values - mean_val
    spread = jnp.mean(centred * centred, axis=1, keepdims=True)
    return (centred * lax.rsqrt(spread + EPSILON) * gain_row).astype(jnp.bfloat16)


def rows_dot(rows, weight_t):
    return lax.dot_general(
        rows, weight_t, (((1,), (1,)), ((), ())), preferred_element_type=jnp.float32
    )


def fused_kernel(
    sizes, x_ref, mask_ref, gin_ref, proj_ref, gate_ref, gout_ref, outw_ref, o_ref,
    x_in, x_out, x_got, p_all, g_all, d_all, gain_own, gain_got, l_send, r_send, part_send, l_got, r_got,
    l_wide, r_wide, turn_a, turn_b, z_out, z_got, gin_own, gout_own, flag_own,
    s_sem, x_sem, ls_sem, rs_sem, lr_sem, rr_sem, copy_sem,
):
    n_gx, n_gy, n_gz, side = sizes
    n_q = n_gy * n_gz
    row_id, gy_id, gz_id = lax.axis_index("gx"), lax.axis_index("gy"), lax.axis_index("gz")
    col_id = gy_id * n_gz + gz_id
    other = 1 - gz_id
    half = x_ref.shape[2]
    full = 2 * half
    pairs = side * side
    on_diag = row_id == col_id
    first = gz_id == 0
    own_rows = pl.ds(pl.multiple_of(gz_id * half, half), half)

    def device(at_row, at_col):
        return {"gx": at_row, "gy": at_col // n_gz, "gz": lax.rem(at_col, n_gz)}

    def push(src, dst, send_sem, recv_sem, to):
        return pltpu.make_async_remote_copy(
            src_ref=src, dst_ref=dst, send_sem=send_sem, recv_sem=recv_sem,
            device_id=to, device_id_type=MESH_ID,
        )

    small = [
        pltpu.make_async_copy(src, dst, copy_sem.at[n])
        for n, (src, dst) in enumerate(((gin_ref, gin_own), (gout_ref, gout_own), (mask_ref, flag_own)), 7)
    ]
    for load in small:
        load.start()
    loads = [
        pltpu.make_async_copy(src, dst, copy_sem.at[n])
        for n, (src, dst) in enumerate((
            (x_ref, x_in),
            (proj_ref.at[0], p_all.at[0, :, own_rows, :]),
            (gate_ref.at[0], g_all.at[0, own_rows, :]),
            (outw_ref.at[0], d_all.at[0, own_rows, :]),
            (proj_ref.at[1], p_all.at[1, :, own_rows, :]),
            (gate_ref.at[1], g_all.at[1, own_rows, :]),
            (outw_ref.at[1], d_all.at[1, own_rows, :]),
        ))
    ]
    for load in loads:
        load.start()
    barrier = pltpu.get_barrier_semaphore()
    for step in range(1, n_gx * n_q):
        peer = lax.rem(row_id * n_q + col_id + step, n_gx * n_q)
        pl.semaphore_signal(
            barrier, inc=1, device_id=device(peer // n_q, lax.rem(peer, n_q)), device_id_type=MESH_ID
        )

    low_lanes = lax.broadcasted_iota(jnp.int32, (pairs, full), 1) < half
    low_packed = low_lanes[: pairs // 2]

    def pack(rows):
        return jnp.where(low_packed, rows[: pairs // 2], pltpu.roll(rows[pairs // 2 :], half, 1))

    def unpack(packed):
        return jnp.concatenate([packed, pltpu.roll(packed, half, 1)], axis=0)

    gain_own[...] = jnp.zeros_like(gain_own)
    for load in small:
        load.wait()
    gain_own[0:2, 0:half] = gin_own[...]
    gain_own[2:4, 0:half] = gout_own[...]
    n_res = mask_ref.shape[1]
    pair_no = lax.broadcasted_iota(jnp.int32, (pairs, n_res), 0)
    residue = lax.broadcasted_iota(jnp.int32, (pairs, n_res), 1)
    in_row = ((pair_no.astype(jnp.float32) + 0.5) / side).astype(jnp.int32)
    in_col = pair_no - in_row * side
    flags = flag_own[...].astype(jnp.float32)
    row_flag = jnp.sum(jnp.where(residue == in_row + row_id * side, flags, 0.0), axis=1, keepdims=True)
    col_flag = jnp.sum(jnp.where(residue == in_col + col_id * side, flags, 0.0), axis=1, keepdims=True)
    mask = row_flag * col_flag

    mate = {"gz": other}
    swaps = [
        push(src, dst, s_sem.at[n], x_sem.at[n], mate)
        for n, (src, dst) in enumerate((
            (x_out, x_got),
            (gain_own, gain_got),
            (proj_ref.at[0], p_all.at[0, :, own_rows, :]),
            (gate_ref.at[0], g_all.at[0, own_rows, :]),
            (outw_ref.at[0], d_all.at[0, own_rows, :]),
            (proj_ref.at[1], p_all.at[1, :, own_rows, :]),
            (gate_ref.at[1], g_all.at[1, own_rows, :]),
            (outw_ref.at[1], d_all.at[1, own_rows, :]),
        ))
    ]
    pl.semaphore_wait(barrier, n_gx * n_q - 1)
    swaps[2].start()
    swaps[1].start()
    loads[0].wait()
    turn_a[...] = jnp.zeros_like(turn_a)
    turn_b[...] = jnp.zeros_like(turn_b)
    for i in range(side):
        left_cols, right_cols = x_in[i, 0:side, :], x_in[i, side : 2 * side, :]
        turn_a[pl.ds(i * side, side), 0:half] = jnp.where(first, left_cols, right_cols)
        turn_b[pl.ds(i * side, side), 0:half] = jnp.where(first, right_cols, left_cols)
    x_out[...] = pack(turn_b[...])

    swaps[0].start()
    for swap in swaps[3:]:
        swap.start()
    swaps[0].wait()
    swaps[1].wait()

    def merge(mine, theirs, lanes):
        low, high = jnp.where(first, mine, theirs), jnp.where(first, theirs, mine)
        return jnp.where(lanes, low, pltpu.roll(high, half, 1))

    gains = merge(gain_own[...], gain_got[...], low_lanes[0:8])
    current = merge(turn_a[...], unpack(x_got[...]), low_lanes)

    for u in range(2):
        normed = channel_norm(current, gains[u : u + 1])
        loads[1 + 3 * u].wait()
        swaps[2 + 3 * u].wait()
        def gated(side_no):
            projected = rows_dot(normed, p_all[u, 2 * side_no : 2 * side_no + 2].reshape(2 * full, full))
            return jax.nn.sigmoid(projected[:, :full]) * projected[:, full:] * mask

        def side_sends(what, targets):
            src, dst, send_sems, recv_sems = what
            for t, (to, guard) in enumerate(targets):
                copy = push(src, dst, send_sems.at[u, t], recv_sems, to)
                if guard is None:
                    copy.start()
                else:
                    pl.when(guard)(copy.start)
                sent.append((guard, copy))

        def block_product(totals, left_row):
            fresh = list(totals)
            for k in range(side):
                right_k = r_wide[pl.ds(k * side, side), :]
                for i in range(side):
                    fresh[i] = fresh[i] + l_wide[pl.ds(left_row(k, i), 1), :] * right_k
            return fresh

        def late_weights():
            for n in (1, 2):
                loads[1 + 3 * u + n].wait()
                swaps[2 + 3 * u + n].wait()
            return jax.nn.sigmoid(rows_dot(normed, g_all[u]))

        sent = []
        plane = [
            lax.rem(gy_id + t // n_gz, n_gy) * n_gz + lax.rem(gz_id + t, n_gz) for t in range(n_q)
        ]
        in_plane = [(device(row_id, at), None) for at in plane[:0:-1]]
        zeros = [jnp.zeros((side, full), jnp.float32) for _ in range(side)]
        if u == 0:
            right_end = row_id >= n_gx // 2
            far_rows = [jnp.where(right_end, t, n_gx - 1 - t) for t in range(n_gx)]
            turn_a[...] = gated(1)
            for k in range(side):
                turn_b[pl.ds(k * side, side), :] = turn_a[pl.ds(k, side, stride=side), :]
            r_send[...] = turn_b[...].astype(jnp.bfloat16)
            side_sends(
                (r_send, r_got.at[u, col_id], rs_sem, rr_sem.at[u, col_id]),
                [(device(t, row_id), jnp.logical_not(on_diag & (row_id == t))) for t in far_rows],
            )
            l_send[u] = gated(0).astype(jnp.bfloat16)
            side_sends((l_send.at[u], l_got.at[u, col_id], ls_sem, lr_sem.at[u, col_id]), in_plane)
            gate = late_weights()
            totals = zeros
            for t, slot in enumerate(plane):
                l_in = push(l_send.at[u], l_got.at[u, slot], ls_sem.at[u, 0], lr_sem.at[u, slot], mate)
                r_in = push(r_send, r_got.at[u, slot], rs_sem.at[u, 0], rr_sem.at[u, slot], mate)
                if t == 0:
                    l_wide[...] = l_send[u].astype(jnp.float32)

                    @pl.when(on_diag)
                    def _():
                        r_got[u, slot] = r_send[...]

                    pl.when(jnp.logical_not(on_diag))(r_in.wait_recv)
                else:
                    l_in.wait_recv()
                    r_in.wait_recv()
                    l_wide[...] = l_got[u, slot].astype(jnp.float32)
                r_wide[...] = r_got[u, slot].astype(jnp.float32)
                totals = block_product(totals, lambda k, i: i * side + k)
            for i in range(side):
                turn_a[pl.ds(i * side, side), :] = totals[i]
        else:
            l_send[u] = gated(0).astype(jnp.bfloat16)
            side_sends((l_send.at[u], l_got.at[u, col_id], ls_sem, lr_sem.at[u, col_id]), in_plane)
            r_wide[...] = gated(1).astype(jnp.bfloat16).astype(jnp.float32)
            gate = late_weights()
            for t, slot in enumerate(plane):
                if t == 0:
                    l_wide[...] = l_send[u].astype(jnp.float32)
                else:
                    push(l_send.at[u], l_got.at[u, slot], ls_sem.at[u, 0], lr_sem.at[u, slot], mate).wait_recv()
                    l_wide[...] = l_got[u, slot].astype(jnp.float32)
                totals = block_product(zeros, lambda k, i: k * side + i)
                for i in range(side):
                    turn_b[pl.ds(i * side, side), :] = totals[i]
                part_send[t] = turn_b[...].astype(jnp.bfloat16)

                @pl.when(slot == row_id)
                def _():
                    turn_a[...] = turn_b[...]

                copy = push(
                    part_send.at[t], r_got.at[u, row_id], rs_sem.at[u, t], rr_sem.at[u, row_id],
                    device(slot, col_id),
                )
                pl.when(slot != row_id)(copy.start)
                sent.append((slot != row_id, copy))
            for t in range(1, n_gx):
                slot = lax.rem(row_id + t, n_gx)
                push(part_send.at[0], r_got.at[u, slot], rs_sem.at[u, 0], rr_sem.at[u, slot], mate).wait_recv()
                turn_a[...] += r_got[u, slot].astype(jnp.float32)
        tri_normed = channel_norm(turn_a[...], gains[2 + u : 3 + u])
        current = current + gate * rows_dot(tri_normed, d_all[u])
        for guard, copy in sent:
            if guard is None:
                copy.wait_send()
            else:
                pl.when(guard)(copy.wait_send)

    turned = pltpu.roll(current, half, 1)
    z_out[...] = pack(jnp.where(first, turned, current))
    back = push(z_out, z_got, s_sem.at[8], x_sem.at[8], mate)
    back.start()
    turn_a[...] = jnp.where(first, current, turned)
    back.wait()
    turn_b[...] = unpack(z_got[...])
    for i in range(side):
        mine, theirs = turn_a[pl.ds(i * side, side), 0:half], turn_b[pl.ds(i * side, side), 0:half]
        x_in[i, 0:side, :] = jnp.where(first, mine, theirs)
        x_in[i, side : 2 * side, :] = jnp.where(first, theirs, mine)
    result = pltpu.make_async_copy(x_in, o_ref, copy_sem.at[0])
    result.start()
    result.wait()


def fused_device(
    sizes, pair, residue_mask, norm_in_gain, proj_weight, gate_weight, norm_out_gain, out_weight
):
    n_gx, n_gy, n_gz, side = sizes
    half = pair.shape[0]
    full = 2 * half
    pairs = side * side
    n_q = n_gy * n_gz
    hbm = pl.BlockSpec(memory_space=pl.ANY)
    dma = pltpu.SemaphoreType.DMA
    blocks = pltpu.VMEM((2, n_q, pairs, full), jnp.bfloat16)
    block = pltpu.VMEM((pairs, full), jnp.float32)
    packed = pltpu.VMEM((pairs // 2, full), jnp.float32)
    out = pl.pallas_call(
        functools.partial(fused_kernel, sizes),
        out_shape=jax.ShapeDtypeStruct((side, n_gz * side, half), jnp.float32),
        in_specs=[hbm] * 7,
        out_specs=hbm,
        scratch_shapes=[
            pltpu.VMEM((side, n_gz * side, half), jnp.float32),
            packed,
            packed,
            pltpu.VMEM((2, 4, full, full), jnp.bfloat16),
            pltpu.VMEM((2, full, full), jnp.bfloat16),
            pltpu.VMEM((2, full, full), jnp.bfloat16),
            pltpu.VMEM((8, full), jnp.float32),
            pltpu.VMEM((8, full), jnp.float32),
            pltpu.VMEM((2, pairs, full), jnp.bfloat16),
            pltpu.VMEM((pairs, full), jnp.bfloat16),
            pltpu.VMEM((n_q, pairs, full), jnp.bfloat16),
            blocks, blocks,
            block, block, block, block,
            packed, packed,
            pltpu.VMEM(norm_in_gain.shape, jnp.float32),
            pltpu.VMEM(norm_out_gain.shape, jnp.float32),
            pltpu.VMEM((1, residue_mask.shape[0]), jnp.int32),
            dma((9,)), dma((9,)),
            dma((2, n_q)), dma((2, n_q)), dma((2, n_q)), dma((2, n_q)),
            dma((10,)),
        ],
        compiler_params=pltpu.CompilerParams(collective_id=0, has_side_effects=True),
    )(
        jnp.transpose(pair, (1, 2, 0)),
        residue_mask[None, :],
        norm_in_gain,
        jnp.transpose(proj_weight, (0, 1, 3, 2)),
        jnp.transpose(gate_weight, (0, 2, 1)),
        norm_out_gain,
        jnp.transpose(out_weight, (0, 2, 1)),
    )
    return jnp.transpose(out, (2, 0, 1))


def solution(mesh):
    n_gx, n_gy, n_gz = (mesh.shape[name] for name in ("gx", "gy", "gz"))

    def step(pair, *rest):
        _, rows, cols = pair.shape
        square = n_gz == 2 and n_gx == n_gy * n_gz and cols == n_gz * rows and rows % 4 == 0
        if square:
            return fused_device((n_gx, n_gy, n_gz, rows), pair, *rest)
        return per_device(pair, *rest)

    return jax.shard_map(
        step,
        mesh=mesh,
        in_specs=(
            P(("groups", "gz"), "gx", "gy"),
            P("groups"),
            P(None, "gz"),
            P(None, None, None, "gz"),
            P(None, None, "gz"),
            P(None, "gz"),
            P(None, None, "gz"),
        ),
        out_specs=P(("groups", "gz"), "gx", "gy"),
        check_vma=False,
    )
```
